32 devices in a mesh: seq: 8 (over z, y), head: 4 (over x, core).
Axes of the slice: x: 2, y: 2, z: 4, core: 2. Of those that a mesh axis runs over, the one named last changes fastest.
Arguments:
- queries: bfloat16 [4096, 2048], P('seq', 'head'), may hold values from -6 to 6
- key_vectors: bfloat16 [4096, 2048], P('seq', 'head'), may hold values from -6 to 6
- value_vectors: bfloat16 [4096, 2048], P('seq', 'head'), may hold values from -6 to 6
- gate_input: bfloat16 [4096, 2048], P('seq', 'head'), may hold values from -6 to 6
- out_weight: bfloat16 [2048, 4096], P('seq', 'head'), may hold values from -0.125 to 0.125
Outputs:
- layer_output: bfloat16 [4096, 4096], P('seq', 'head')
The draws below stay inside these ranges and needn't reach their ends.
All inputs are finite; a program needn't handle non-finite values.
Results may differ from the reference program's by a relative error of at most 0.0057.
Values may be sent and summed in bfloat16 or wider, within the bound.
A program may use at most 64 MiB of HBM per device.

```python
import jax
import jax.numpy as jnp
from jax import lax

D = 4096
HD = 128
H = 16
TOK_DEV = 512
TOKENS = 4096


def block_levels(rng, shape, shards, smallest, largest):
    def one(position, blocks):
        draws = jax.random.uniform(jax.random.fold_in(jax.random.fold_in(rng, 6), position), (blocks,), jnp.float32, smallest / len(shards), largest / len(shards))
        return jnp.repeat(jnp.exp(draws), shape[position] // blocks).reshape((-1,) + (1,) * (len(shape) - position - 1))

    level = one(*shards[0])
    for cut in shards[1:]:
        level = level * one(*cut)
    return level


def normal_values(key, dims, scale, most, shards=(), kind=jnp.bfloat16):
    level = block_levels(key, dims, shards, -0.22, 0.18) if shards else 1.0
    values = jax.random.normal(key, dims, jnp.float32) * scale * level
    return jnp.minimum(jnp.maximum(values, -most), most).astype(kind)


def setup_inputs(seed: int = 0) -> dict:
    key_of = jax.random.split(jax.random.key(seed), 6)
    return {
        "queries": normal_values(key_of[0], (TOKENS, H * HD), 1.0, 6.0, ((0, 8), (1, 4))),
        "key_vectors": normal_values(key_of[1], (TOKENS, H * HD), 1.0, 6.0, ((0, 8), (1, 4))),
        "value_vectors": normal_values(key_of[2], (TOKENS, H * HD), 1.0, 6.0, ((0, 8), (1, 4))),
        "gate_input": normal_values(key_of[3], (TOKENS, H * HD), 1.0, 6.0, ((0, 8), (1, 4))),
        "out_weight": normal_values(key_of[4], (H * HD, D), (H * HD) ** -0.5, 0.125, ((0, 8), (1, 4))),
    }


def reference(queries, key_vectors, value_vectors, gate_input, out_weight):
    scale = HD ** (-0.5)
    blocks = TOKENS // TOK_DEV

    def shaped(array):
        return array.reshape(blocks, TOK_DEV, H * HD)
    rowpos = lax.broadcasted_iota(jnp.int32, (TOK_DEV, TOK_DEV), 0)
    colpos = lax.broadcasted_iota(jnp.int32, (TOK_DEV, TOK_DEV), 1)
    causal = colpos <= rowpos

    def block_step(carry, inputs):
        query_blk, key_blk, value_blk, gate_blk = inputs
        qhead = query_blk.reshape(TOK_DEV, H, HD).astype(jnp.float32)
        khead = key_blk.reshape(TOK_DEV, H, HD).astype(jnp.float32)
        vhead = value_blk.reshape(TOK_DEV, H, HD).astype(jnp.float32)
        scores = jnp.einsum('thd,shd->hts', qhead, khead) * scale
        scores = jnp.where(causal[None, :, :], scores, 0.0).astype(jnp.bfloat16)
        intra = jnp.einsum('hts,she->the', scores.astype(jnp.float32), vhead)
        rounded = carry.astype(jnp.bfloat16).astype(jnp.float32)
        inter = jnp.einsum('thd,hde->the', qhead, rounded) * scale
        attn = (intra + inter).reshape(TOK_DEV, H * HD)
        state = jnp.einsum('thd,the->hde', khead, vhead)
        mean_square = lax.optimization_barrier(jnp.mean(attn * attn, axis=1))
        hidden = (attn * jax.nn.silu(gate_blk.astype(jnp.float32))).astype(jnp.bfloat16)
        projected = jnp.dot(hidden, out_weight, preferred_element_type=jnp.float32)
        result = (projected * lax.rsqrt(mean_square + 1e-06)[:, None]).astype(jnp.bfloat16)
        return (carry + state, result)
    start = jnp.zeros((H, HD, HD), jnp.float32)
    final, outputs = lax.scan(block_step, start, (shaped(queries), shaped(key_vectors), shaped(value_vectors), shaped(gate_input)))
    return outputs.reshape(TOKENS, D)
```

```python
import functools

import jax
import jax.numpy as jnp
from jax import lax
from jax.experimental import pallas as pl
from jax.experimental.pallas import tpu as pltpu
from jax.sharding import PartitionSpec as P

HD = 128
PIECES = 2
LONGEST_LINE = 8
MESH = pl.DeviceIdType.MESH
F32 = jnp.float32
BF16 = jnp.bfloat16


def dot(a, b, dims):
    return lax.dot_general(a, b, (dims, ((), ())), preferred_element_type=F32)


def fused_kernel(
    n, m,
    q_hbm, k_hbm, v_hbm, g_hbm, w_hbm, out_ref,
    q_ref, k_ref, v_ref, g_ref, w_all, hid, attn, own_state, s_out, s_in, t_out, t_in, prefix,
    sq, acc,
    load_sem, w_recv, up_send, down_send, side_send,
    s_send, s_recv, t_send, t_recv, h_send, h_recv, q_send, q_recv,
):
    rows, width = q_ref.shape
    heads = width // HD
    scale = HD ** (-0.5)
    depth = w_all.shape[1]
    piece = depth // PIECES
    per_peer = width // depth
    line = n // 2
    me = lax.axis_index("seq")
    hx = lax.axis_index("head")
    z = me // 2
    y = me % 2
    partner = z * 2 + (1 - y)

    loads = [
        pltpu.make_async_copy(src, dst, load_sem.at[i])
        for i, (src, dst) in enumerate(
            ((k_hbm, k_ref), (v_hbm, v_ref), (w_hbm, w_all.at[me]), (q_hbm, q_ref), (g_hbm, g_ref))
        )
    ]
    for load in loads:
        load.start()

    barrier = pltpu.get_barrier_semaphore()
    for d in range(1, line):
        other = ((z + d) % line) * 2 + y
        pl.semaphore_signal(barrier, inc=1, device_id={"seq": other}, device_id_type=MESH)
    pl.semaphore_signal(barrier, inc=1, device_id={"seq": partner}, device_id_type=MESH)
    for d in range(1, m):
        pl.semaphore_signal(barrier, inc=1, device_id={"head": (hx + d) % m}, device_id_type=MESH)

    def w_copy(block, c, send_sems, target):
        part = w_all.at[block, pl.ds(c * piece, piece), :]
        return pltpu.make_async_remote_copy(
            src_ref=part, dst_ref=part,
            send_sem=send_sems.at[block, c], recv_sem=w_recv.at[block, c],
            device_id={"seq": target}, device_id_type=MESH,
        )

    def up(block, c):
        return w_copy(block, c, up_send, jnp.minimum(me + 2, n - 1))

    def down(block, c):
        return w_copy(block, c, down_send, jnp.maximum(me - 2, 0))

    def side(block, c):
        return w_copy(block, c, side_send, partner)

    has_up = z < line - 1
    has_down = z > 0

    loads[0].wait()
    loads[1].wait()
    for h in range(heads):
        cols = slice(h * HD, (h + 1) * HD)
        state = dot(k_ref[:, cols], v_ref[:, cols], ((0,), (0,)))
        own_state[cols, :] = state
        s_out[cols, :] = state.astype(BF16)
    loads[2].wait()
    pl.semaphore_wait(barrier, line - 1 + 1 + m - 1)

    s_copy = pltpu.make_async_remote_copy(
        src_ref=s_out, dst_ref=s_in, send_sem=s_send, recv_sem=s_recv,
        device_id={"seq": partner}, device_id_type=MESH,
    )
    s_copy.start()

    @pl.when(has_down)
    def _():
        for c in range(PIECES):
            down(me, c).start()

    @pl.when(has_up)
    def _():
        up(me, 0).start()

    for c in range(PIECES):
        side(me, c).start()

    loads[3].wait()

    def local_head(h):
        cols = slice(h * HD, (h + 1) * HD)
        kh = k_ref[:, cols]
        vh = v_ref[:, cols]
        half = rows // 2
        for r in range(2):
            upto = (r + 1) * half
            scores = dot(q_ref[r * half:upto, cols], kh[:upto], ((1,), (1,))) * scale
            rowpos = r * half + lax.broadcasted_iota(jnp.int32, (half, upto), 0)
            colpos = lax.broadcasted_iota(jnp.int32, (half, upto), 1)
            scores = jnp.where(colpos <= rowpos, scores, 0.0).astype(BF16)
            attn[r * half:upto, cols] = dot(scores, vh[:upto], ((1,), (0,)))

    local_head(0)

    s_copy.wait_recv()
    t_out[...] = (own_state[...] + s_in[...].astype(F32)).astype(BF16)

    def t_copy(source, target):
        return pltpu.make_async_remote_copy(
            src_ref=t_out, dst_ref=t_in.at[source],
            send_sem=t_send.at[target], recv_sem=t_recv.at[source],
            device_id={"seq": target * 2 + y}, device_id_type=MESH,
        )

    for target in range(line - 1, 0, -1):
        @pl.when(target > z)
        def _():
            t_copy(z, target).start()

    @pl.when(has_up)
    def _():
        for c in range(1, PIECES):
            up(me, c).start()

    for h in range(1, heads):
        local_head(h)
    prefix[...] = jnp.where(y == 1, s_in[...].astype(F32), 0.0)

    def pass_down(step, c):
        @pl.when(z + step <= line - 1)
        def _():
            block = me + 2 * step
            side(block, c).wait_recv()

            @pl.when(has_down)
            def _():
                down(block, c).start()
            side(block, c).start()

    def pass_up(step, c):
        @pl.when(z >= step)
        def _():
            block = me - 2 * step
            side(block, c).wait_recv()

            @pl.when(has_up)
            def _():
                up(block, c).start()
            side(block, c).start()

    pass_down(1, 0)

    for source in range(line - 1):
        @pl.when(source < z)
        def _():
            t_copy(source, z).wait_recv()
            prefix[...] += t_in[source].astype(F32)

    loads[4].wait()
    total = jnp.zeros((rows, 1), F32)
    for h in range(heads):
        cols = slice(h * HD, (h + 1) * HD)
        inter = dot(q_ref[:, cols], prefix[cols, :].astype(BF16), ((1,), (0,))) * scale
        value = attn[:, cols] + inter
        total = total + jnp.sum(value * value, axis=1, keepdims=True)
        gate = g_ref[:, cols].astype(F32)
        gated = (value * (gate / (1.0 + jnp.exp(-gate)))).astype(BF16)
        block, offset = divmod(h * HD, depth)
        hid[hx * per_peer + block, :, offset:offset + HD] = gated
    sq[hx] = jnp.broadcast_to(total, (rows, HD)).T[:8]

    peers = [(hx + d) % m for d in range(1, m)]

    def h_copy(d):
        part = hid.at[pl.ds(hx * per_peer, per_peer)]
        return pltpu.make_async_remote_copy(
            src_ref=part, dst_ref=part, send_sem=h_send.at[d], recv_sem=h_recv.at[hx],
            device_id={"head": peers[d]}, device_id_type=MESH,
        )

    def q_copy(d):
        return pltpu.make_async_remote_copy(
            src_ref=sq.at[hx], dst_ref=sq.at[hx], send_sem=q_send.at[d], recv_sem=q_recv.at[hx],
            device_id={"head": peers[d]}, device_id_type=MESH,
        )

    for d in range(m - 1):
        q_copy(d).start()
        h_copy(d).start()

    for c in range(1, PIECES):
        pass_down(1, c)
    for c in range(PIECES):
        pass_up(1, c)
    for step in range(2, line):
        for c in range(PIECES):
            pass_down(step, c)
            pass_up(step, c)

    for d in range(m - 1):
        source = peers[d]
        part = hid.at[pl.ds(source * per_peer, per_peer)]
        pltpu.make_async_remote_copy(
            src_ref=part, dst_ref=part, send_sem=h_send.at[d], recv_sem=h_recv.at[source],
            device_id={"head": source}, device_id_type=MESH,
        ).wait_recv()
        pltpu.make_async_remote_copy(
            src_ref=sq.at[source], dst_ref=sq.at[source], send_sem=q_send.at[d],
            recv_sem=q_recv.at[source], device_id={"head": source}, device_id_type=MESH,
        ).wait_recv()
    squares = sq[0]
    for i in range(1, m):
        squares = squares + sq[i]
    inverse = lax.rsqrt(squares / (m * width) + 1e-06)
    inverse = jnp.broadcast_to(inverse[:1], (HD, rows)).T[:, :1]

    acc[...] = jnp.zeros_like(acc)
    low = z < line // 2

    def place(j):
        return jnp.where(low, (z + j) % line, (z + line - j) % line)

    def own_column(j, carry):
        block = place(j) * 2 + y
        acc[...] += dot(hid[block], w_all[block], ((1,), (0,)))
        return carry

    lax.fori_loop(0, line, own_column, 0)

    def other_column(j, carry):
        block = place(j) * 2 + (1 - y)
        for c in range(PIECES):
            side(block, c).wait_recv()
        acc[...] += dot(hid[block], w_all[block], ((1,), (0,)))
        return carry

    lax.fori_loop(0, line, other_column, 0)
    out_ref[...] = (acc[...] * inverse).astype(out_ref.dtype)

    s_copy.wait_send()
    for target in range(1, line):
        @pl.when(target > z)
        def _():
            t_copy(z, target).wait_send()
    for d in range(m - 1):
        h_copy(d).wait_send()
        q_copy(d).wait_send()
    for zb in range(line):
        block = zb * 2 + y

        @pl.when((zb <= z) & has_up)
        def _():
            for c in range(PIECES):
                up(block, c).wait_send()

        @pl.when((zb >= z) & has_down)
        def _():
            for c in range(PIECES):
                down(block, c).wait_send()
        for c in range(PIECES):
            side(block, c).wait_send()


def fused(n, m, queries, key_vectors, value_vectors, gate_input, out_weight):
    rows, width = queries.shape
    depth, columns = out_weight.shape
    line = n // 2
    dma = pltpu.SemaphoreType.DMA
    return pl.pallas_call(
        functools.partial(fused_kernel, n, m),
        out_shape=jax.ShapeDtypeStruct((rows, columns), BF16),
        in_specs=[pl.BlockSpec(memory_space=pl.ANY)] * 5,
        out_specs=pl.BlockSpec(memory_space=pltpu.VMEM),
        scratch_shapes=[
            pltpu.VMEM((rows, width), BF16),
            pltpu.VMEM((rows, width), BF16),
            pltpu.VMEM((rows, width), BF16),
            pltpu.VMEM((rows, width), BF16),
            pltpu.VMEM((n, depth, columns), BF16),
            pltpu.VMEM((n, rows, depth), BF16),
            pltpu.VMEM((rows, width), F32),
            pltpu.VMEM((width, HD), F32),
            pltpu.VMEM((width, HD), BF16),
            pltpu.VMEM((width, HD), BF16),
            pltpu.VMEM((width, HD), BF16),
            pltpu.VMEM((line, width, HD), BF16),
            pltpu.VMEM((width, HD), F32),
            pltpu.VMEM((m, 8, rows), F32),
            pltpu.VMEM((rows, columns), F32),
            dma((5,)),
            dma((n, PIECES)),
            dma((n, PIECES)),
            dma((n, PIECES)),
            dma((n, PIECES)),
            dma,
            dma,
            dma((line,)),
            dma((line,)),
            dma((m,)),
            dma((m,)),
            dma((m,)),
            dma((m,)),
        ],
        compiler_params=pltpu.CompilerParams(
            collective_id=0, has_side_effects=True, vmem_limit_bytes=48 * 1024 * 1024
        ),
        cost_estimate=pl.CostEstimate(
            flops=2 * rows * n * depth * columns, bytes_accessed=2 * n * depth * columns,
            transcendentals=rows * width,
        ),
    )(queries, key_vectors, value_vectors, gate_input, out_weight)


def long_line(queries, key_vectors, value_vectors, gate_input, out_weight):
    rows, width = queries.shape
    heads = width // HD
    scale = HD ** (-0.5)
    qhead = queries.reshape(rows, heads, HD)
    khead = key_vectors.reshape(rows, heads, HD)
    vhead = value_vectors.reshape(rows, heads, HD)
    own_state = jnp.einsum("thd,the->hde", khead, vhead, preferred_element_type=F32)
    scores = jnp.einsum("thd,shd->hts", qhead, khead, preferred_element_type=F32) * scale
    rowpos = lax.broadcasted_iota(jnp.int32, (rows, rows), 0)
    colpos = lax.broadcasted_iota(jnp.int32, (rows, rows), 1)
    scores = jnp.where((colpos <= rowpos)[None, :, :], scores, 0.0).astype(BF16)
    local = jnp.einsum("hts,she->the", scores, vhead, preferred_element_type=F32)
    states = lax.all_gather(own_state, "seq")
    position = lax.axis_index("seq")

    def turn(k, before):
        return jnp.where(k < position, before + states[k], before)

    prefix = lax.fori_loop(0, lax.axis_size("seq"), turn, jnp.zeros_like(own_state))
    inter = jnp.einsum("thd,hde->the", qhead, prefix.astype(BF16), preferred_element_type=F32)
    attn = (local + inter * scale).reshape(rows, width)
    total = lax.psum(jnp.sum(attn * attn, axis=1), "head")
    hidden = (attn * jax.nn.silu(gate_input.astype(F32))).astype(BF16)
    features = lax.all_gather(hidden, "head", axis=1, tiled=True)
    weights = lax.all_gather(out_weight, "seq", axis=0, tiled=True)
    projected = jnp.dot(features, weights, preferred_element_type=F32)
    mean_square = total / features.shape[1]
    return (projected * lax.rsqrt(mean_square + 1e-06)[:, None]).astype(BF16)


def solution(mesh):
    n, m = mesh.shape["seq"], mesh.shape["head"]

    def per_device(queries, key_vectors, value_vectors, gate_input, out_weight):
        args = (queries, key_vectors, value_vectors, gate_input, out_weight)
        width, depth = queries.shape[1], out_weight.shape[0]
        short = n % 2 == 0 and n // 2 <= LONGEST_LINE
        if short and width % depth == 0 and depth % HD == 0:
            return fused(n, m, *args)
        return long_line(*args)

    placed = (P("seq", "head"),) * 5
    return jax.shard_map(
        per_device, mesh=mesh, in_specs=placed, out_specs=P("seq", "head"), check_vma=False
    )
```

```python
import functools

import jax
import jax.numpy as jnp
from jax import lax
from jax.experimental import pallas as pl
from jax.experimental.pallas import tpu as pltpu
from jax.sharding import PartitionSpec as P

HD = 128
PIECES = 4
CROSS_DOWN = 1
CROSS_UP = 0
LONGEST_LINE = 8
MESH = pl.DeviceIdType.MESH
F32 = jnp.float32
BF16 = jnp.bfloat16


def dot(a, b, dims):
    return lax.dot_general(a, b, (dims, ((), ())), preferred_element_type=F32)


def fused_kernel(
    n, m,
    q_hbm, k_hbm, v_hbm, g_hbm, w_hbm, out_ref,
    q_ref, k_ref, v_ref, g_ref, w_all, hid, attn, own_state, s_out, s_in, t_out, t_in, prefix,
    sq, acc,
    load_sem, w_recv, up_send, down_send, side_send,
    s_send, s_recv, t_send, t_recv, h_send, h_recv, q_send, q_recv,
):
    rows, width = q_ref.shape
    heads = width // HD
    scale = HD ** (-0.5)
    depth = w_all.shape[1]
    piece = depth // PIECES
    per_peer = width // depth
    line = n // 2
    me = lax.axis_index("seq")
    hx = lax.axis_index("head")
    z = me // 2
    y = me % 2
    partner = z * 2 + (1 - y)

    loads = [
        pltpu.make_async_copy(src, dst, load_sem.at[i])
        for i, (src, dst) in enumerate(
            ((w_hbm, w_all.at[me]), (k_hbm, k_ref), (v_hbm, v_ref), (q_hbm, q_ref), (g_hbm, g_ref))
        )
    ]
    for load in loads:
        load.start()

    barrier = pltpu.get_barrier_semaphore()
    above = jnp.where(z == line - 1, y, me + 2)
    below = jnp.where(z == 0, n - 2 + y, me - 2)
    for other in (above, below):
        pl.semaphore_signal(barrier, inc=1, device_id={"seq": other}, device_id_type=MESH)
    pl.semaphore_signal(barrier, inc=1, device_id={"seq": partner}, device_id_type=MESH)
    for d in range(1, m):
        pl.semaphore_signal(barrier, inc=1, device_id={"head": (hx + d) % m}, device_id_type=MESH)

    def w_copy(block, c, send_sems, target):
        part = w_all.at[block, pl.ds(c * piece, piece), :]
        return pltpu.make_async_remote_copy(
            src_ref=part, dst_ref=part,
            send_sem=send_sems.at[block, c], recv_sem=w_recv.at[block, c],
            device_id={"seq": target}, device_id_type=MESH,
        )

    def up(block, c):
        return w_copy(block, c, up_send, jnp.minimum(me + 2, n - 1))

    def down(block, c):
        return w_copy(block, c, down_send, jnp.maximum(me - 2, 0))

    def side(block, c):
        return w_copy(block, c, side_send, partner)

    order = tuple(reversed(range(PIECES)))
    cross_down, cross_up = order[:CROSS_DOWN], order[:CROSS_UP]
    crossing = order[:max(CROSS_DOWN, CROSS_UP)]
    has_up = z < line - 1
    has_down = z > 0

    early = PIECES // 2
    ahead = PIECES // 4
    loads[0].wait()
    pl.semaphore_wait(barrier, 3 + m - 1)
    for c in order[:ahead]:
        side(me, c).start()

    @pl.when(has_down)
    def _():
        for c in order:
            down(me, c).start()

    @pl.when(has_up)
    def _():
        for c in order[:early]:
            up(me, c).start()

    @pl.when(has_up & has_down)
    def _():
        for c in order[early:]:
            up(me, c).start()

    loads[1].wait()
    loads[2].wait()
    for h in range(heads):
        cols = slice(h * HD, (h + 1) * HD)
        state = dot(k_ref[:, cols], v_ref[:, cols], ((0,), (0,)))
        own_state[cols, :] = state
        s_out[cols, :] = state.astype(BF16)

    s_copy = pltpu.make_async_remote_copy(
        src_ref=s_out, dst_ref=s_in, send_sem=s_send, recv_sem=s_recv,
        device_id={"seq": partner}, device_id_type=MESH,
    )
    s_copy.start()
    for c in order[ahead:]:
        side(me, c).start()

    loads[3].wait()

    def local_head(h):
        cols = slice(h * HD, (h + 1) * HD)
        kh = k_ref[:, cols]
        vh = v_ref[:, cols]
        half = rows // 2
        for r in range(2):
            upto = (r + 1) * half
            scores = dot(q_ref[r * half:upto, cols], kh[:upto], ((1,), (1,))) * scale
            rowpos = r * half + lax.broadcasted_iota(jnp.int32, (half, upto), 0)
            colpos = lax.broadcasted_iota(jnp.int32, (half, upto), 1)
            scores = jnp.where(colpos <= rowpos, scores, 0.0).astype(BF16)
            attn[r * half:upto, cols] = dot(scores, vh[:upto], ((1,), (0,)))

    local_head(0)

    s_copy.wait_recv()
    t_copy = pltpu.make_async_remote_copy(
        src_ref=t_out, dst_ref=t_in, send_sem=t_send, recv_sem=t_recv,
        device_id={"seq": jnp.minimum(me + 2, n - 1)}, device_id_type=MESH,
    )

    @pl.when(z == 0)
    def _():
        t_out[...] = (own_state[...] + s_in[...].astype(F32)).astype(BF16)
        t_copy.start()
        for c in order[early:]:
            up(me, c).start()

    for h in range(1, heads):
        local_head(h)
    prefix[...] = jnp.where(y == 1, s_in[...].astype(F32), 0.0)

    def pass_down(step, c, own):
        @pl.when(z + step <= line - 1)
        def _():
            block = (z + step) * 2 + (y if own else 1 - y)
            side(block, c).wait_recv()

            @pl.when(has_down)
            def _():
                down(block, c).start()
            if c not in cross_down:
                side(block, c).start()

    def pass_up(step, c, own):
        @pl.when(z >= step)
        def _():
            block = (z - step) * 2 + (y if own else 1 - y)
            side(block, c).wait_recv()

            @pl.when(has_up)
            def _():
                up(block, c).start()
            if c not in cross_up:
                side(block, c).start()

    def turn_off(c):
        side(partner, c).wait_recv()
        if c in cross_down:
            @pl.when(has_down)
            def _():
                down(partner, c).start()
        if c in cross_up:
            @pl.when(has_up)
            def _():
                up(partner, c).start()

    def pass_both(step, c):
        pass_down(step, c, True)
        pass_up(step, c, True)
        if c in cross_down:
            pass_down(step, c, False)
        if c in cross_up:
            pass_up(step, c, False)

    for c in order[:early]:
        pass_down(1, c, True)

    @pl.when(z >= 2)
    def _():
        for c in order[:ahead]:
            pass_up(1, c, True)

    @pl.when(has_down)
    def _():
        t_copy.wait_recv()

        @pl.when(has_up)
        def _():
            t_out[...] = (
                t_in[...].astype(F32) + own_state[...] + s_in[...].astype(F32)
            ).astype(BF16)
            t_copy.start()
        prefix[...] += t_in[...].astype(F32)

    loads[4].wait()
    total = jnp.zeros((rows, 1), F32)
    for h in range(heads):
        cols = slice(h * HD, (h + 1) * HD)
        inter = dot(q_ref[:, cols], prefix[cols, :].astype(BF16), ((1,), (0,))) * scale
        value = attn[:, cols] + inter
        total = total + jnp.sum(value * value, axis=1, keepdims=True)
        gate = g_ref[:, cols].astype(F32)
        gated = (value * (gate / (1.0 + jnp.exp(-gate)))).astype(BF16)
        block, offset = divmod(h * HD, depth)
        hid[hx * per_peer + block, :, offset:offset + HD] = gated
    sq[hx] = jnp.broadcast_to(total, (rows, HD)).T[:8]

    peers = [(hx + d) % m for d in range(1, m)]

    mate = hx + 1 - 2 * (hx % 2)
    pairs = m // 2

    def h_copy(source, target, i):
        part = hid.at[pl.ds(source * per_peer, per_peer)]
        return pltpu.make_async_remote_copy(
            src_ref=part, dst_ref=part, send_sem=h_send.at[i], recv_sem=h_recv.at[source],
            device_id={"head": target}, device_id_type=MESH,
        )

    def q_copy(source, d):
        return pltpu.make_async_remote_copy(
            src_ref=sq.at[source], dst_ref=sq.at[source], send_sem=q_send.at[d],
            recv_sem=q_recv.at[source], device_id={"head": peers[d]}, device_id_type=MESH,
        )

    h_sends = [h_copy(hx, (hx + 2 * d) % m, d) for d in range(1, pairs)] + [h_copy(hx, mate, 0)]
    q_sends = [q_copy(hx, d) for d in range(m - 1)]
    for send in q_sends + h_sends:
        send.start()

    for c in crossing:
        turn_off(c)

    @pl.when(z < 2)
    def _():
        for c in order[:ahead]:
            pass_up(1, c, True)
    for c in order[ahead:early]:
        pass_up(1, c, True)
    for c in order[early:]:
        pass_down(1, c, True)
        pass_up(1, c, True)
    for c in cross_down:
        pass_down(1, c, False)
    for c in cross_up:
        pass_up(1, c, False)
    for step in range(2, line - 1):
        for c in order:
            pass_both(step, c)

    relays = []
    for d in range(1, pairs):
        source = (hx + 2 * d) % m
        relay = h_copy(source, mate, pairs + d)
        relay.wait_recv()
        relay.start()
        relays.append(relay)
    for d in range(pairs):
        h_copy((mate + 2 * d) % m, mate, 0).wait_recv()
    for d in range(m - 1):
        q_copy(peers[d], d).wait_recv()
    squares = sq[0]
    for i in range(1, m):
        squares = squares + sq[i]
    inverse = lax.rsqrt(squares / (m * width) + 1e-06)
    inverse = jnp.broadcast_to(inverse[:1], (HD, rows)).T[:, :1]

    near = jnp.minimum(z, line - 1 - z)

    def place(j):
        d = (j + 1) // 2
        alternate = z + d if j % 2 else z - d
        beyond = jnp.where(z < line // 2, j, line - 1 - j)
        return jnp.where(j <= 2 * near, alternate, beyond)

    def wait_side(zb):
        block = zb * 2 + (1 - y)
        for where, crossed in ((zb > z, cross_down), (zb == z, crossing), (zb < z, cross_up)):
            @pl.when(where)
            def _():
                for c in order:
                    if c not in crossed:
                        side(block, c).wait_recv()

    def add_block(block):
        acc[...] += dot(hid[block], w_all[block], ((1,), (0,)))

    block = me
    acc[...] = dot(hid[block], w_all[block], ((1,), (0,)))
    for j in range(1, line):
        if j == line - 1:
            for c in order[(line - 2) * ahead:]:
                pass_both(line - 1, c)
        else:
            for c in order[(j - 1) * ahead:j * ahead]:
                pass_both(line - 1, c)
        add_block(place(j) * 2 + y)
    for j in range(line):
        block = place(j) * 2 + (1 - y)
        wait_side(place(j))
        add_block(block)
    out_ref[...] = (acc[...] * inverse).astype(out_ref.dtype)

    s_copy.wait_send()

    @pl.when(has_up)
    def _():
        t_copy.wait_send()
    for send in q_sends + h_sends + relays:
        send.wait_send()
    for zb in range(line):
        for column, ups, downs in ((y, order, order), (1 - y, cross_up, cross_down)):
            block = zb * 2 + column

            @pl.when((zb <= z) & has_up)
            def _():
                for c in ups:
                    up(block, c).wait_send()

            @pl.when((zb >= z) & has_down)
            def _():
                for c in downs:
                    down(block, c).wait_send()
        for where, crossed in ((zb > z, cross_down), (zb == z, ()), (zb < z, cross_up)):
            @pl.when(where)
            def _():
                for c in order:
                    if c not in crossed:
                        side(zb * 2 + y, c).wait_send()


def fused(n, m, queries, key_vectors, value_vectors, gate_input, out_weight):
    rows, width = queries.shape
    depth, columns = out_weight.shape
    line = n // 2
    dma = pltpu.SemaphoreType.DMA
    return pl.pallas_call(
        functools.partial(fused_kernel, n, m),
        out_shape=jax.ShapeDtypeStruct((rows, columns), BF16),
        in_specs=[pl.BlockSpec(memory_space=pltpu.HBM)] * 5,
        out_specs=pl.BlockSpec(memory_space=pltpu.VMEM),
        scratch_shapes=[
            pltpu.VMEM((rows, width), BF16),
            pltpu.VMEM((rows, width), BF16),
            pltpu.VMEM((rows, width), BF16),
            pltpu.VMEM((rows, width), BF16),
            pltpu.VMEM((n, depth, columns), BF16),
            pltpu.VMEM((n, rows, depth), BF16),
            pltpu.VMEM((rows, width), F32),
            pltpu.VMEM((width, HD), F32),
            pltpu.VMEM((width, HD), BF16),
            pltpu.VMEM((width, HD), BF16),
            pltpu.VMEM((width, HD), BF16),
            pltpu.VMEM((width, HD), BF16),
            pltpu.VMEM((width, HD), F32),
            pltpu.VMEM((m, 8, rows), F32),
            pltpu.VMEM((rows, columns), F32),
            dma((5,)),
            dma((n, PIECES)),
            dma((n, PIECES)),
            dma((n, PIECES)),
            dma((n, PIECES)),
            dma,
            dma,
            dma,
            dma,
            dma((m,)),
            dma((m,)),
            dma((m,)),
            dma((m,)),
        ],
        compiler_params=pltpu.CompilerParams(
            collective_id=0, has_side_effects=True, vmem_limit_bytes=57000 * 1024
        ),
        cost_estimate=pl.CostEstimate(
            flops=2 * rows * n * depth * columns, bytes_accessed=2 * n * depth * columns,
            transcendentals=rows * width,
        ),
    )(queries, key_vectors, value_vectors, gate_input, out_weight)


def long_line(queries, key_vectors, value_vectors, gate_input, out_weight):
    rows, width = queries.shape
    heads = width // HD
    scale = HD ** (-0.5)
    qhead = queries.reshape(rows, heads, HD)
    khead = key_vectors.reshape(rows, heads, HD)
    vhead = value_vectors.reshape(rows, heads, HD)
    own_state = jnp.einsum("thd,the->hde", khead, vhead, preferred_element_type=F32)
    scores = jnp.einsum("thd,shd->hts", qhead, khead, preferred_element_type=F32) * scale
    rowpos = lax.broadcasted_iota(jnp.int32, (rows, rows), 0)
    colpos = lax.broadcasted_iota(jnp.int32, (rows, rows), 1)
    scores = jnp.where((colpos <= rowpos)[None, :, :], scores, 0.0).astype(BF16)
    local = jnp.einsum("hts,she->the", scores, vhead, preferred_element_type=F32)
    states = lax.all_gather(own_state, "seq")
    position = lax.axis_index("seq")

    def turn(k, before):
        return jnp.where(k < position, before + states[k], before)

    prefix = lax.fori_loop(0, lax.axis_size("seq"), turn, jnp.zeros_like(own_state))
    inter = jnp.einsum("thd,hde->the", qhead, prefix.astype(BF16), preferred_element_type=F32)
    attn = (local + inter * scale).reshape(rows, width)
    total = lax.psum(jnp.sum(attn * attn, axis=1), "head")
    hidden = (attn * jax.nn.silu(gate_input.astype(F32))).astype(BF16)
    features = lax.all_gather(hidden, "head", axis=1, tiled=True)
    weights = lax.all_gather(out_weight, "seq", axis=0, tiled=True)
    projected = jnp.dot(features, weights, preferred_element_type=F32)
    mean_square = total / features.shape[1]
    return (projected * lax.rsqrt(mean_square + 1e-06)[:, None]).astype(BF16)


def solution(mesh):
    n, m = mesh.shape["seq"], mesh.shape["head"]

    def per_device(queries, key_vectors, value_vectors, gate_input, out_weight):
        args = (queries, key_vectors, value_vectors, gate_input, out_weight)
        width, depth = queries.shape[1], out_weight.shape[0]
        short = n % 2 == 0 and m % 2 == 0 and 3 <= n // 2 <= LONGEST_LINE
        if short and width % depth == 0 and depth % HD == 0:
            return fused(n, m, *args)
        return long_line(*args)

    placed = (P("seq", "head"),) * 5
    return jax.shard_map(
        per_device, mesh=mesh, in_specs=placed, out_specs=P("seq", "head"), check_vma=False
    )
```

```python
import functools

import jax
import jax.numpy as jnp
from jax import lax
from jax.experimental import pallas as pl
from jax.experimental.pallas import tpu as pltpu
from jax.sharding import PartitionSpec as P

HD = 128
PIECES = 4
CROSS_DOWN = 1
CROSS_UP = 0
LONGEST_LINE = 8
MESH = pl.DeviceIdType.MESH
F32 = jnp.float32
BF16 = jnp.bfloat16


def dot(a, b, dims):
    return lax.dot_general(a, b, (dims, ((), ())), preferred_element_type=F32)


def fused_kernel(
    n, m,
    q_hbm, k_hbm, v_hbm, g_hbm, w_hbm, out_ref,
    q_ref, k_ref, v_ref, g_ref, w_all, hid, attn, own_state, s_out, s_in, t_out, t_in, prefix,
    sq, acc,
    load_sem, w_recv, up_send, down_send, side_send,
    s_send, s_recv, t_send, t_recv, h_send, h_recv, q_send, q_recv,
):
    rows, width = q_ref.shape
    heads = width // HD
    scale = HD ** (-0.5)
    depth = w_all.shape[1]
    piece = depth // PIECES
    per_peer = width // depth
    line = n // 2
    me = lax.axis_index("seq")
    hx = lax.axis_index("head")
    z = me // 2
    y = me % 2
    partner = z * 2 + (1 - y)

    loads = [
        pltpu.make_async_copy(src, dst, load_sem.at[i])
        for i, (src, dst) in enumerate(
            ((w_hbm, w_all.at[me]), (k_hbm, k_ref), (v_hbm, v_ref), (q_hbm, q_ref), (g_hbm, g_ref))
        )
    ]
    for load in loads:
        load.start()

    barrier = pltpu.get_barrier_semaphore()
    above = jnp.where(z == line - 1, y, me + 2)
    below = jnp.where(z == 0, n - 2 + y, me - 2)
    for other in (above, below):
        pl.semaphore_signal(barrier, inc=1, device_id={"seq": other}, device_id_type=MESH)
    pl.semaphore_signal(barrier, inc=1, device_id={"seq": partner}, device_id_type=MESH)
    for d in range(1, m):
        pl.semaphore_signal(barrier, inc=1, device_id={"head": (hx + d) % m}, device_id_type=MESH)

    def w_copy(block, c, send_sems, target):
        part = w_all.at[block, pl.ds(c * piece, piece), :]
        return pltpu.make_async_remote_copy(
            src_ref=part, dst_ref=part,
            send_sem=send_sems.at[block, c], recv_sem=w_recv.at[block, c],
            device_id={"seq": target}, device_id_type=MESH,
        )

    def up(block, c):
        return w_copy(block, c, up_send, jnp.minimum(me + 2, n - 1))

    def down(block, c):
        return w_copy(block, c, down_send, jnp.maximum(me - 2, 0))

    def side(block, c):
        return w_copy(block, c, side_send, partner)

    order = tuple(reversed(range(PIECES)))
    cross_down, cross_up = order[:CROSS_DOWN], order[:CROSS_UP]
    crossing = order[:max(CROSS_DOWN, CROSS_UP)]
    has_up = z < line - 1
    has_down = z > 0

    early = PIECES // 2
    ahead = PIECES // 4
    loads[0].wait()
    pl.semaphore_wait(barrier, 3 + m - 1)
    for c in order[:ahead]:
        side(me, c).start()

    @pl.when(has_down)
    def _():
        for c in order:
            down(me, c).start()

    @pl.when(has_up)
    def _():
        for c in order[:early]:
            up(me, c).start()

    @pl.when(has_up & has_down)
    def _():
        for c in order[early:]:
            up(me, c).start()

    loads[1].wait()
    loads[2].wait()
    for h in range(heads):
        cols = slice(h * HD, (h + 1) * HD)
        state = dot(k_ref[:, cols], v_ref[:, cols], ((0,), (0,)))
        own_state[cols, :] = state
        s_out[cols, :] = state.astype(BF16)

    s_copy = pltpu.make_async_remote_copy(
        src_ref=s_out, dst_ref=s_in, send_sem=s_send, recv_sem=s_recv,
        device_id={"seq": partner}, device_id_type=MESH,
    )
    s_copy.start()
    for c in order[ahead:]:
        side(me, c).start()

    loads[3].wait()

    def local_head(h):
        cols = slice(h * HD, (h + 1) * HD)
        kh = k_ref[:, cols]
        vh = v_ref[:, cols]
        half = rows // 2
        for r in range(2):
            upto = (r + 1) * half
            scores = dot(q_ref[r * half:upto, cols], kh[:upto], ((1,), (1,))) * scale
            rowpos = r * half + lax.broadcasted_iota(jnp.int32, (half, upto), 0)
            colpos = lax.broadcasted_iota(jnp.int32, (half, upto), 1)
            scores = jnp.where(colpos <= rowpos, scores, 0.0).astype(BF16)
            attn[r * half:upto, cols] = dot(scores, vh[:upto], ((1,), (0,)))

    local_head(0)

    s_copy.wait_recv()
    t_copy = pltpu.make_async_remote_copy(
        src_ref=t_out, dst_ref=t_in, send_sem=t_send, recv_sem=t_recv,
        device_id={"seq": jnp.minimum(me + 2, n - 1)}, device_id_type=MESH,
    )

    @pl.when(z == 0)
    def _():
        t_out[...] = (own_state[...] + s_in[...].astype(F32)).astype(BF16)
        t_copy.start()
        for c in order[early:]:
            up(me, c).start()

    for h in range(1, heads):
        local_head(h)
    prefix[...] = jnp.where(y == 1, s_in[...].astype(F32), 0.0)

    def pass_down(step, c, own):
        @pl.when(z + step <= line - 1)
        def _():
            block = (z + step) * 2 + (y if own else 1 - y)
            side(block, c).wait_recv()

            @pl.when(has_down)
            def _():
                down(block, c).start()
            if c not in cross_down:
                side(block, c).start()

    def pass_up(step, c, own):
        @pl.when(z >= step)
        def _():
            block = (z - step) * 2 + (y if own else 1 - y)
            side(block, c).wait_recv()

            @pl.when(has_up)
            def _():
                up(block, c).start()
            if c not in cross_up:
                side(block, c).start()

    def turn_off(c):
        side(partner, c).wait_recv()
        if c in cross_down:
            @pl.when(has_down)
            def _():
                down(partner, c).start()
        if c in cross_up:
            @pl.when(has_up)
            def _():
                up(partner, c).start()

    def pass_both(step, c):
        pass_down(step, c, True)
        pass_up(step, c, True)
        if c in cross_down:
            pass_down(step, c, False)
        if c in cross_up:
            pass_up(step, c, False)

    for c in order[:early]:
        pass_down(1, c, True)

    @pl.when(z >= 2)
    def _():
        for c in order[early:]:
            pass_down(1, c, True)
        for c in order[:ahead]:
            pass_up(1, c, True)

    @pl.when(z == line - 1)
    def _():
        for c in order[ahead:]:
            pass_up(1, c, True)

    @pl.when(has_down)
    def _():
        t_copy.wait_recv()

        @pl.when(has_up)
        def _():
            t_out[...] = (
                t_in[...].astype(F32) + own_state[...] + s_in[...].astype(F32)
            ).astype(BF16)
            t_copy.start()
        prefix[...] += t_in[...].astype(F32)

    loads[4].wait()
    total = jnp.zeros((rows, 1), F32)
    for h in range(heads):
        cols = slice(h * HD, (h + 1) * HD)
        inter = dot(q_ref[:, cols], prefix[cols, :].astype(BF16), ((1,), (0,))) * scale
        value = attn[:, cols] + inter
        total = total + jnp.sum(value * value, axis=1, keepdims=True)
        gate = g_ref[:, cols].astype(F32)
        gated = (value * (gate / (1.0 + jnp.exp(-gate)))).astype(BF16)
        block, offset = divmod(h * HD, depth)
        hid[hx * per_peer + block, :, offset:offset + HD] = gated
    sq[hx] = jnp.broadcast_to(total, (rows, HD)).T[:8]

    peers = [(hx + d) % m for d in range(1, m)]

    mate = hx + 1 - 2 * (hx % 2)
    pairs = m // 2

    def h_copy(source, target, i):
        part = hid.at[pl.ds(source * per_peer, per_peer)]
        return pltpu.make_async_remote_copy(
            src_ref=part, dst_ref=part, send_sem=h_send.at[i], recv_sem=h_recv.at[source],
            device_id={"head": target}, device_id_type=MESH,
        )

    def q_copy(source, d):
        return pltpu.make_async_remote_copy(
            src_ref=sq.at[source], dst_ref=sq.at[source], send_sem=q_send.at[d],
            recv_sem=q_recv.at[source], device_id={"head": peers[d]}, device_id_type=MESH,
        )

    h_sends = [h_copy(hx, (hx + 2 * d) % m, d) for d in range(1, pairs)] + [h_copy(hx, mate, 0)]
    q_sends = [q_copy(hx, d) for d in range(m - 1)]
    for send in q_sends + h_sends:
        send.start()

    for c in crossing:
        turn_off(c)

    @pl.when(z < 2)
    def _():
        for c in order[:ahead]:
            pass_up(1, c, True)
        for c in order[early:]:
            pass_down(1, c, True)

    @pl.when(has_up)
    def _():
        for c in order[ahead:]:
            pass_up(1, c, True)
    for c in cross_down:
        pass_down(1, c, False)
    for c in cross_up:
        pass_up(1, c, False)
    for step in range(2, line - 1):
        for c in order:
            pass_both(step, c)

    relays = []
    for d in range(1, pairs):
        source = (hx + 2 * d) % m
        relay = h_copy(source, mate, pairs + d)
        relay.wait_recv()
        relay.start()
        relays.append(relay)
    for d in range(pairs):
        h_copy((mate + 2 * d) % m, mate, 0).wait_recv()
    for d in range(m - 1):
        q_copy(peers[d], d).wait_recv()
    squares = sq[0]
    for i in range(1, m):
        squares = squares + sq[i]
    inverse = lax.rsqrt(squares / (m * width) + 1e-06)
    inverse = jnp.broadcast_to(inverse[:1], (HD, rows)).T[:, :1]

    near = jnp.minimum(z, line - 1 - z)

    def place(j):
        d = (j + 1) // 2
        alternate = z + d if j % 2 else z - d
        beyond = jnp.where(z < line // 2, j, line - 1 - j)
        return jnp.where(j <= 2 * near, alternate, beyond)

    def wait_side(zb):
        block = zb * 2 + (1 - y)
        for where, crossed in ((zb > z, cross_down), (zb == z, crossing), (zb < z, cross_up)):
            @pl.when(where)
            def _():
                for c in order:
                    if c not in crossed:
                        side(block, c).wait_recv()

    def add_block(block):
        acc[...] += dot(hid[block], w_all[block], ((1,), (0,)))

    block = me
    acc[...] = dot(hid[block], w_all[block], ((1,), (0,)))
    for j in range(1, line):
        if j == line - 1:
            for c in order[(line - 2) * ahead:]:
                pass_both(line - 1, c)
        else:
            for c in order[(j - 1) * ahead:j * ahead]:
                pass_both(line - 1, c)
        add_block(place(j) * 2 + y)
    for j in range(line):
        block = place(j) * 2 + (1 - y)
        wait_side(place(j))
        add_block(block)
    out_ref[...] = (acc[...] * inverse).astype(out_ref.dtype)

    s_copy.wait_send()

    @pl.when(has_up)
    def _():
        t_copy.wait_send()
    for send in q_sends + h_sends + relays:
        send.wait_send()
    for zb in range(line):
        for column, ups, downs in ((y, order, order), (1 - y, cross_up, cross_down)):
            block = zb * 2 + column

            @pl.when((zb <= z) & has_up)
            def _():
                for c in ups:
                    up(block, c).wait_send()

            @pl.when((zb >= z) & has_down)
            def _():
                for c in downs:
                    down(block, c).wait_send()
        for where, crossed in ((zb > z, cross_down), (zb == z, ()), (zb < z, cross_up)):
            @pl.when(where)
            def _():
                for c in order:
                    if c not in crossed:
                        side(zb * 2 + y, c).wait_send()


def fused(n, m, queries, key_vectors, value_vectors, gate_input, out_weight):
    rows, width = queries.shape
    depth, columns = out_weight.shape
    line = n // 2
    dma = pltpu.SemaphoreType.DMA
    return pl.pallas_call(
        functools.partial(fused_kernel, n, m),
        out_shape=jax.ShapeDtypeStruct((rows, columns), BF16),
        in_specs=[pl.BlockSpec(memory_space=pltpu.HBM)] * 5,
        out_specs=pl.BlockSpec(memory_space=pltpu.VMEM),
        scratch_shapes=[
            pltpu.VMEM((rows, width), BF16),
            pltpu.VMEM((rows, width), BF16),
            pltpu.VMEM((rows, width), BF16),
            pltpu.VMEM((rows, width), BF16),
            pltpu.VMEM((n, depth, columns), BF16),
            pltpu.VMEM((n, rows, depth), BF16),
            pltpu.VMEM((rows, width), F32),
            pltpu.VMEM((width, HD), F32),
            pltpu.VMEM((width, HD), BF16),
            pltpu.VMEM((width, HD), BF16),
            pltpu.VMEM((width, HD), BF16),
            pltpu.VMEM((width, HD), BF16),
            pltpu.VMEM((width, HD), F32),
            pltpu.VMEM((m, 8, rows), F32),
            pltpu.VMEM((rows, columns), F32),
            dma((5,)),
            dma((n, PIECES)),
            dma((n, PIECES)),
            dma((n, PIECES)),
            dma((n, PIECES)),
            dma,
            dma,
            dma,
            dma,
            dma((m,)),
            dma((m,)),
            dma((m,)),
            dma((m,)),
        ],
        compiler_params=pltpu.CompilerParams(
            collective_id=0, has_side_effects=True, vmem_limit_bytes=57000 * 1024
        ),
        cost_estimate=pl.CostEstimate(
            flops=2 * rows * n * depth * columns, bytes_accessed=2 * n * depth * columns,
            transcendentals=rows * width,
        ),
    )(queries, key_vectors, value_vectors, gate_input, out_weight)


def long_line(queries, key_vectors, value_vectors, gate_input, out_weight):
    rows, width = queries.shape
    heads = width // HD
    scale = HD ** (-0.5)
    qhead = queries.reshape(rows, heads, HD)
    khead = key_vectors.reshape(rows, heads, HD)
    vhead = value_vectors.reshape(rows, heads, HD)
    own_state = jnp.einsum("thd,the->hde", khead, vhead, preferred_element_type=F32)
    scores = jnp.einsum("thd,shd->hts", qhead, khead, preferred_element_type=F32) * scale
    rowpos = lax.broadcasted_iota(jnp.int32, (rows, rows), 0)
    colpos = lax.broadcasted_iota(jnp.int32, (rows, rows), 1)
    scores = jnp.where((colpos <= rowpos)[None, :, :], scores, 0.0).astype(BF16)
    local = jnp.einsum("hts,she->the", scores, vhead, preferred_element_type=F32)
    states = lax.all_gather(own_state, "seq")
    position = lax.axis_index("seq")

    def turn(k, before):
        return jnp.where(k < position, before + states[k], before)

    prefix = lax.fori_loop(0, lax.axis_size("seq"), turn, jnp.zeros_like(own_state))
    inter = jnp.einsum("thd,hde->the", qhead, prefix.astype(BF16), preferred_element_type=F32)
    attn = (local + inter * scale).reshape(rows, width)
    total = lax.psum(jnp.sum(attn * attn, axis=1), "head")
    hidden = (attn * jax.nn.silu(gate_input.astype(F32))).astype(BF16)
    features = lax.all_gather(hidden, "head", axis=1, tiled=True)
    weights = lax.all_gather(out_weight, "seq", axis=0, tiled=True)
    projected = jnp.dot(features, weights, preferred_element_type=F32)
    mean_square = total / features.shape[1]
    return (projected * lax.rsqrt(mean_square + 1e-06)[:, None]).astype(BF16)


def solution(mesh):
    n, m = mesh.shape["seq"], mesh.shape["head"]

    def per_device(queries, key_vectors, value_vectors, gate_input, out_weight):
        args = (queries, key_vectors, value_vectors, gate_input, out_weight)
        width, depth = queries.shape[1], out_weight.shape[0]
        short = n % 2 == 0 and m % 2 == 0 and 3 <= n // 2 <= LONGEST_LINE
        if short and width % depth == 0 and depth % HD == 0:
            return fused(n, m, *args)
        return long_line(*args)

    placed = (P("seq", "head"),) * 5
    return jax.shard_map(
        per_device, mesh=mesh, in_specs=placed, out_specs=P("seq", "head"), check_vma=False
    )
```
